32 devices in a mesh: leaf: 8 (over z, y), front: 4 (over x, core).
Axes of the slice: x: 2, y: 2, z: 4, core: 2. Of those that a mesh axis runs over, the one named last changes fastest.
Arguments:
- app_rhs: float32 [24576, 128], P(('leaf', 'front')), may hold values from -6 to 6
- pivot_source: int32 [24576], P(('leaf', 'front')), may hold values from 0 to 24575, as said below
- row_owner: int32 [24576], P(('leaf', 'front')), may hold values from 0 to 24575, as said below
- leaf_inverse: float32 [8, 4, 384, 1536], P('leaf', 'front'), may hold values from -1 to 2, as said below
- leaf_coupling: float32 [8, 4, 384, 1024], P('leaf', 'front'), may hold values from -0.07654656 to 0.07654656
- sep1_inverse: float32 [8, 4, 128, 1024], P('leaf', 'front'), may hold values from -1 to 2, as said below
- sep1_coupling: float32 [8, 4, 128, 2048], P('leaf', 'front'), may hold values from -0.09375 to 0.09375
- sep2_inverse: float32 [8, 4, 128, 2048], P('leaf', 'front'), may hold values from -1 to 2, as said below
- sep2_coupling: float32 [8, 4, 128, 4096], P('leaf', 'front'), may hold values from -0.06629126 to 0.06629126
- sep3_inverse: float32 [8, 4, 128, 4096], P('leaf', 'front'), may hold values from -1 to 2, as said below
Outputs:
- solution: float32 [24576, 128], P(('leaf', 'front'))
The draws below stay inside these ranges and needn't reach their ends.
Inputs may be any that keep to these rules, and one draw needn't show every extreme that they name: `pivot_source`: A permutation. Row e of pivot_rhs comes from a device's block of 768 application rows; one block's rows go to at most 16 blocks of pivot rows, at most 60 rows from one block to one block, and some pair of blocks carries exactly 60 rows. The inverse of pivot_source: pivot_source[row_owner[i]] = i. `leaf_inverse`: each front's matrix is the identity plus dense entries of magnitude at most 2 / sqrt of the front's pivot rows. `sep1_inverse`: as leaf_inverse. `sep2_inverse`: as leaf_inverse. `sep3_inverse`: as leaf_inverse.
All inputs are finite; a program needn't handle non-finite values.
Results may differ from the reference program's by a relative error of at most 0.00011.
Values sent between devices are 32-bit elements; how exact they have to be, the bound alone decides.
A program may use at most 128 MiB of HBM per device.

```python
import jax
import jax.numpy as jnp
from jax import lax

NRHS = 128
LEAF_PIV = 384
SEP_PIV = 128
ROWS_DEV = 768
FANOUT = 16
SPREAD = 12
NROWS = 24576
LEAF_FRONT = 1536
SEP1 = 1024
SEP2 = 2048
SEP3 = 4096
N_LEAF = 8
N_FRONT = 4


def route_tables(key):
    base_key = jax.random.fold_in(key, 7)
    keys_all = jax.random.split(base_key, 6)
    device_count = N_LEAF * N_FRONT
    row_count = ROWS_DEV
    mean_rows = ROWS_DEV // FANOUT
    labels = jax.random.permutation(keys_all[0], device_count)
    turns = jax.random.permutation(keys_all[1], device_count)
    shifts = jax.random.permutation(keys_all[2], device_count)[:FANOUT]
    offsets = jax.random.randint(keys_all[3], (FANOUT // 2,), 0, SPREAD + 1)
    offsets = offsets.at[0].set(SPREAD)
    weights = jnp.stack([mean_rows + offsets, mean_rows - offsets], axis=1).reshape(FANOUT)
    bucket_ends = jnp.cumsum(weights)
    slot_index = jnp.arange(row_count, dtype=jnp.int32)
    bucket = jnp.sum((slot_index[:, None] >= bucket_ends[None, :]).astype(jnp.int32), axis=1)
    label_of = (turns[:, None] + shifts[bucket][None, :]) % device_count
    target = jnp.argsort(labels)[label_of].astype(jnp.int32)
    local_order = jax.vmap(lambda sub_key: jax.random.permutation(sub_key, row_count))(jax.random.split(keys_all[4], device_count))
    app_row = jnp.arange(device_count, dtype=jnp.int32)[:, None] * row_count + local_order.astype(jnp.int32)
    priority = jax.random.permutation(keys_all[5], device_count * row_count).reshape(device_count, row_count).astype(jnp.int32)
    scores = (target * (device_count * row_count) + priority).reshape(-1)
    sorted_items = jnp.argsort(scores, stable=True)
    source_rows = app_row.reshape(-1)[sorted_items].astype(jnp.int32)
    owner_rows = jnp.zeros(device_count * row_count, jnp.int32).at[source_rows].set(jnp.arange(device_count * row_count, dtype=jnp.int32))
    return (source_rows, owner_rows)


def draw_pivot_source(key, part):
    return route_tables(key)[0]


def draw_row_owner(key, part):
    return route_tables(key)[1]


def draw_front(key, group_size, pivot_rows, width):
    full_shape = (N_LEAF, N_FRONT, pivot_rows, width)
    leaf_axis = jnp.arange(N_LEAF)[:, None, None, None]
    front_axis = jnp.arange(N_FRONT)[None, :, None, None]
    pivot_axis = jnp.arange(pivot_rows)[None, None, :, None]
    column_axis = jnp.arange(width)[None, None, None, :]
    diagonal_col = front_axis * (group_size * pivot_rows) + leaf_axis % group_size * pivot_rows + pivot_axis
    identity = (column_axis == diagonal_col).astype(jnp.float32)
    jitter = jnp.clip(jax.random.normal(key, full_shape, jnp.float32), -4.0, 4.0)
    return identity + 0.5 * jitter / width ** 0.5


def draw_leaf_inverse(key, part):
    return draw_front(jax.random.fold_in(key, 11), 1, LEAF_PIV, LEAF_FRONT)


def draw_sep1_inverse(key, part):
    return draw_front(jax.random.fold_in(key, 12), 2, SEP_PIV, SEP1)


def draw_sep2_inverse(key, part):
    return draw_front(jax.random.fold_in(key, 13), 4, SEP_PIV, SEP2)


def draw_sep3_inverse(key, part):
    return draw_front(jax.random.fold_in(key, 14), 8, SEP_PIV, SEP3)


def block_scale(stream_key, extent, cuts, least, high):
    gain, own = 1.0, jax.random.fold_in(stream_key, 6)
    for axis_at, shards_of in cuts:
        draws = jnp.exp(jax.random.uniform(jax.random.fold_in(own, axis_at), (shards_of,), jnp.float32, least / len(cuts), high / len(cuts)))
        gain = gain * jnp.repeat(draws, extent[axis_at] // shards_of).reshape([-1 if axis == axis_at else 1 for axis in range(len(extent))])
    return gain


def noise(own_key, extent, spread, limit, shards=(), kind=jnp.bfloat16):
    gain = block_scale(own_key, extent, shards, -0.22, 0.18) if shards else 1.0
    drawn = jax.random.normal(own_key, extent, jnp.float32) * spread * gain
    return jnp.minimum(jnp.maximum(drawn, -limit), limit).astype(kind)


def setup_inputs(seed: int = 0) -> dict:
    streams_of = jax.random.split(jax.random.key(seed), 11)
    return {
        "app_rhs": noise(streams_of[0], (NROWS, NRHS), 1.0, 6.0, ((0, 32),), jnp.float32),
        "pivot_source": draw_pivot_source(jax.random.fold_in(streams_of[10], 71), 0),
        "row_owner": draw_row_owner(jax.random.fold_in(streams_of[10], 71), 0),
        "leaf_inverse": draw_leaf_inverse(jax.random.fold_in(streams_of[10], 71), 0),
        "leaf_coupling": noise(streams_of[4], (N_LEAF, N_FRONT, LEAF_PIV, SEP1), (0.5 * LEAF_FRONT ** -0.5), 0.07654656, ((0, 8), (1, 4)), jnp.float32),
        "sep1_inverse": draw_sep1_inverse(jax.random.fold_in(streams_of[10], 71), 0),
        "sep1_coupling": noise(streams_of[6], (N_LEAF, N_FRONT, SEP_PIV, SEP2), (0.5 * SEP1 ** -0.5), 0.09375, ((0, 8), (1, 4)), jnp.float32),
        "sep2_inverse": draw_sep2_inverse(jax.random.fold_in(streams_of[10], 71), 0),
        "sep2_coupling": noise(streams_of[8], (N_LEAF, N_FRONT, SEP_PIV, SEP3), (0.5 * SEP2 ** -0.5), 0.06629126, ((0, 8), (1, 4)), jnp.float32),
        "sep3_inverse": draw_sep3_inverse(jax.random.fold_in(streams_of[10], 71), 0),
    }


PRECISE = lax.Precision.HIGHEST


def node_form(blocked, group_size):
    leaves, fronts, pivot_rows, col_count = blocked.shape
    shaped = blocked.reshape(leaves // group_size, group_size, fronts, pivot_rows, col_count)
    shaped = jnp.transpose(shaped, (0, 2, 1, 3, 4))
    return shaped.reshape(leaves // group_size, fronts * group_size * pivot_rows, col_count)


def device_form(nodes, group_size, fronts, pivot_rows):
    node_count, row_count, col_count = nodes.shape
    shaped = nodes.reshape(node_count, fronts, group_size, pivot_rows, col_count)
    shaped = jnp.transpose(shaped, (0, 2, 1, 3, 4))
    return shaped.reshape(node_count * group_size, fronts, pivot_rows, col_count)


def apply_rows(matrices, vectors):
    return jnp.einsum("nab,nbc->nac", matrices, vectors, precision=PRECISE)


def apply_cols(matrices, vectors):
    return jnp.einsum("nba,nbc->nac", matrices, vectors, precision=PRECISE)


def pair_sum(partials):
    node_count, row_count, col_count = partials.shape
    return partials.reshape(node_count // 2, 2, row_count, col_count).sum(axis=1)


def reference(app_rhs, pivot_source, row_owner, leaf_inverse, leaf_coupling, sep1_inverse, sep1_coupling, sep2_inverse, sep2_coupling, sep3_inverse):
    leaves = leaf_inverse.shape[0]
    fronts = leaf_inverse.shape[1]
    ordered = app_rhs[pivot_source].reshape(leaves, fronts, ROWS_DEV, NRHS)
    inverses = [leaf_inverse, sep1_inverse, sep2_inverse, sep3_inverse]
    couplings = [leaf_coupling, sep1_coupling, sep2_coupling]
    pivots = [LEAF_PIV, SEP_PIV, SEP_PIV, SEP_PIV]
    starts = [0, LEAF_PIV, LEAF_PIV + SEP_PIV, LEAF_PIV + 2 * SEP_PIV]
    solved = []
    carried = None
    for height in range(4):
        group_size = 2 ** height
        own_rhs = node_form(ordered[:, :, starts[height]:starts[height] + pivots[height]], group_size)
        if height > 0:
            own_rhs = own_rhs - carried
        forward = apply_rows(node_form(inverses[height], group_size), own_rhs)
        solved.append(forward)
        if height < 3:
            carried = pair_sum(apply_cols(node_form(couplings[height], group_size), forward))
    pieces = [None, None, None, None]
    parent_sol = None
    for height in (3, 2, 1, 0):
        group_size = 2 ** height
        target = solved[height]
        if height < 3:
            target = target - apply_rows(node_form(couplings[height], group_size), jnp.repeat(parent_sol, 2, axis=0))
        parent_sol = apply_cols(node_form(inverses[height], group_size), target)
        pieces[height] = device_form(parent_sol, group_size, fronts, pivots[height])
    pivot_order = jnp.concatenate(pieces, axis=2).reshape(leaves * fronts * ROWS_DEV, NRHS)
    return pivot_order[row_owner]
```

```python
import functools

import jax
import jax.numpy as jnp
from jax import lax
from jax.experimental import pallas as pl
from jax.experimental.pallas import tpu as pltpu
from jax.sharding import PartitionSpec as P

BLK = 128
HEIGHTS = 4
CLASSES = 3
MESH = pl.DeviceIdType.MESH
CORE = ("front", 0)
STRIPE_UNITS = (3, 3, 3, 2, 2, 3)


def bit_of(value, place):
    return lax.rem(lax.div(value, jnp.int32(2**place)), jnp.int32(2))


def flipped(value, mask, bits):
    out = jnp.int32(0)
    for place in range(bits):
        out = out + lax.rem(bit_of(value, place) + bit_of(mask, place), jnp.int32(2)) * 2**place
    return out


def group_dims(front_bits, height):
    return [("front", place) for place in range(1, front_bits)] + [("leaf", place) for place in range(height)]


def group_orders(front_bits, height):
    dims = group_dims(front_bits, height)
    turns = min(CLASSES, len(dims))
    head, rest = dims[:turns], dims[turns:]
    return [head[turn:] + head[:turn] + rest for turn in range(turns)]


def place_slot(place, height, order):
    slot = 0
    for axis, at in order:
        slot = slot * 2 + (place >> (at + height if axis == "front" else at) & 1)
    return slot


def place_lane(place):
    return bin(place).count("1") % 2


def split(value):
    high = value.astype(jnp.bfloat16)
    return high, (value - high.astype(jnp.float32)).astype(jnp.bfloat16)


def dot(left, right, right_axis):
    dims = (((1,), (right_axis,)), ((), ()))
    return lax.dot_general(left, right, dimension_numbers=dims, preferred_element_type=jnp.float32)


def solve_kernel(leaf_bits, front_bits, stripe_rows, pivots, sizes, cap, *refs):
    app_ref, pack_idx, order_idx, back_pack_idx, back_idx = refs[:5]
    weights_hbm = refs[5:12]
    out_ref = refs[12]
    packed, arrived, returned, ordered, sol = refs[13:18]
    stages = refs[18]
    stacked = refs[19:26]
    left_ref = refs[26]
    solved = refs[27:31]
    buffers = refs[31:-7]
    load_sems, send_sems, recv_sems, go_send, go_recv, back_send, back_recv = refs[-7:]
    stripes = len(stripe_rows)
    lows = [sum(stripe_rows[:s]) for s in range(stripes)]
    pos = 0

    def take(count):
        nonlocal pos
        pos += count
        return buffers[pos - count : pos]

    partial = [take(stripes) for _ in range(HEIGHTS)]
    recv = [take(stripes) for _ in range(HEIGHTS)]
    whole_vec = [partial[0]] + [take(stripes) for _ in range(HEIGHTS - 1)]
    used = [0]

    leaf = lax.axis_index("leaf")
    front = lax.axis_index("front")
    fronts = 2**front_bits
    peers = 2 ** (front_bits + leaf_bits)
    here = {"leaf": leaf, "front": front}
    me = leaf * fronts + front

    def mine(dim):
        return bit_of(here[dim[0]], dim[1])

    core_flip = front + (1 - 2 * mine(CORE))

    def partner(dim):
        axis, place = dim
        if dim == CORE:
            return (leaf, core_flip)
        move = (1 - 2 * mine(dim)) * 2**place
        return (leaf + move, core_flip) if axis == "leaf" else (leaf, core_flip + move)

    def peer(step):
        turn = jnp.int32(peers - 1) - step
        return (
            flipped(leaf, lax.div(turn, jnp.int32(fronts)), leaf_bits),
            flipped(front, lax.rem(turn, jnp.int32(fronts)), front_bits),
        )

    piece_of = [pivots[h] // BLK for h in range(HEIGHTS)]
    halves = [size // BLK // 2 for size in sizes]
    orders = [group_orders(front_bits, h) for h in range(HEIGHTS)]
    lanes = []
    for height in range(HEIGHTS):
        total = jnp.int32(0)
        for place in range(front_bits):
            total = total + bit_of(front, place)
        for place in range(height):
            total = total + bit_of(leaf, place)
        lanes.append(lax.rem(total, jnp.int32(2)))

    def kind(height, stripe):
        return stripe % len(orders[height])

    perms = []
    for height in range(HEIGHTS):
        table = [[0] * halves[height] for _ in orders[height]]
        for place in range(2 ** (front_bits + height)):
            canon = place_slot(place, height, orders[height][0])
            for k, order in enumerate(orders[height]):
                for part in range(piece_of[height]):
                    table[k][canon * piece_of[height] + part] = (
                        place_slot(place, height, order) * piece_of[height] + part
                    )
        perms.append(table)

    weight_heights = (0, 1, 1, 2, 2, 3, 3)
    pieces = []
    for index in range(7):
        for part in range(weights_hbm[index].shape[0] // BLK):
            pieces.append((index, part))

    def stage_copy(number):
        index, part = pieces[number]
        return pltpu.make_async_copy(
            weights_hbm[index].at[pl.ds(part * BLK, BLK)],
            stages.at[number % 2, :, pl.ds(0, weights_hbm[index].shape[1])],
            load_sems.at[number % 2],
        )

    stage_copy(0).start()
    stage_copy(1).start()

    barrier = pltpu.get_barrier_semaphore()

    def greet(step, carry):
        pl.semaphore_signal(barrier, inc=1, device_id=peer(step), device_id_type=MESH)
        return carry

    lax.fori_loop(0, peers - 1, greet, 0)

    def pack_rows(index, source, target, base, where):
        for row in range(cap):
            target[base + row] = source(index[where + row])

    def send_to(step, source, target, sends, recvs):
        to_leaf, to_front = peer(step)
        there = to_leaf * fronts + to_front
        return pltpu.make_async_remote_copy(
            src_ref=source.at[pl.ds(there * cap, cap)],
            dst_ref=target.at[pl.ds(me * cap, cap)],
            send_sem=sends.at[step],
            recv_sem=recvs.at[step],
            device_id=(to_leaf, to_front),
            device_id_type=MESH,
        )

    def exchange_rows(index, source, target, sends, recvs, ready):
        def pack(step):
            to_leaf, to_front = peer(step)
            base = (to_leaf * fronts + to_front) * cap
            pack_rows(index, source, packed, base, base)

        pack(jnp.int32(0))
        ready()

        def body(step, carry):
            pack(step)
            send_to(step - 1, packed, target, sends, recvs).start()
            return carry

        lax.fori_loop(1, peers - 1, body, 0)
        pack_rows(index, source, target, me * cap, me * cap)
        send_to(jnp.int32(peers - 2), packed, target, sends, recvs).start()

    def finish_rows(target, sends, recvs):
        def body(step, carry):
            send_to(step, packed, target, sends, recvs).wait()
            return carry

        lax.fori_loop(0, peers - 1, body, 0)

    def unpack_rows(index, source, target):
        def body(group, carry):
            for row in range(8):
                target[group, pl.ds(row, 1), :] = source[index[group * 8 + row]]
            return carry

        lax.fori_loop(0, target.shape[0], body, 0, unroll=2)

    exchange_rows(
        pack_idx,
        lambda i: app_ref[i],
        arrived,
        go_send,
        go_recv,
        lambda: pl.semaphore_wait(barrier, peers - 1),
    )

    for number, (index, part) in enumerate(pieces):
        height = weight_heights[index]
        piece = piece_of[height]
        rows, cols = weights_hbm[index].shape
        stage_copy(number).wait()

        def convert(group, carry, number=number, index=index, part=part, height=height, rows=rows, cols=cols, piece=piece):
            span = pl.ds(pl.multiple_of(group * 16, 16), 16)
            high_rows = pl.ds(pl.multiple_of(part * BLK + group * 16, 16), 16)
            low_rows = pl.ds(pl.multiple_of(rows + part * BLK + group * 16, 16), 16)
            for block in range(cols // BLK):
                place, rest = divmod(block, piece)
                lane = place_lane(place)
                at = place_slot(place, height, orders[height][0]) * piece + rest
                high, low = split(stages[number % 2, span, pl.ds(block * BLK, BLK)])
                stacked[index][lane, high_rows, pl.ds(at * BLK, BLK)] = high
                stacked[index][lane, low_rows, pl.ds(at * BLK, BLK)] = low
            return carry

        lax.fori_loop(0, BLK // 16, convert, 0)
        if number + 2 < len(pieces):
            stage_copy(number + 2).start()

    finish_rows(arrived, go_send, go_recv)
    unpack_rows(order_idx, arrived, ordered)

    def remote(source, target, dim):
        index = used[0]
        used[0] += 1
        copy = pltpu.make_async_remote_copy(
            src_ref=source,
            dst_ref=target,
            send_sem=send_sems.at[index],
            recv_sem=recv_sems.at[index],
            device_id=partner(dim),
            device_id_type=MESH,
        )
        copy.start()
        return copy

    def own_slots(height):
        out = []
        for stripe in range(stripes):
            slot = jnp.int32(0)
            for dim in orders[height][kind(height, stripe)]:
                slot = slot * 2 + mine(dim)
            out.append(lanes[height] * halves[height] + slot * piece_of[height])
        return out

    def own_block(bufs, slots, part):
        return jnp.concatenate([bufs[s][slots[s] + part] for s in range(stripes)], axis=0)

    def reduce_steps(height, swap_at, fill):
        bufs, recvs, result = partial[height], recv[height], whole_vec[height]
        swap = swap_at is not None
        half = halves[height]
        lane = lanes[height]
        fill(1 - lane)
        pending = [
            remote(bufs[s].at[pl.ds((1 - lane) * half, half)], recvs[s].at[pl.ds(0, half)], CORE)
            for s in range(stripes)
        ]
        fill(lane)
        bases = [lane * half] * stripes
        depth = len(orders[height][0])
        whole, prior, offset = half, 0, half
        for step in range(depth + 1):
            full = swap and step == depth - 1
            size = whole if full else whole // 2
            if full:
                offset = swap_at
            copies = []
            for s in range(stripes):
                pending[s].wait()
                keep = pl.ds(bases[s], whole)
                (result if step == depth else bufs)[s][keep] = bufs[s][keep] + recvs[s][pl.ds(prior, whole)]
                if step < depth:
                    dim = orders[height][kind(height, s)][step]
                    away = bases[s]
                    if not full:
                        away = bases[s] + (1 - mine(dim)) * size
                        bases[s] = bases[s] + mine(dim) * size
                    copies.append(remote(bufs[s].at[pl.ds(away, size)], recvs[s].at[pl.ds(offset, size)], dim))
            pending, prior, whole = copies, offset, size
            offset += size
        return bases

    def gather_steps(height, bufs, bases, size, depth, middle):
        half = halves[height]
        pending = None
        for step in range(depth - 1, -2, -1):
            copies = []
            for s in range(stripes):
                if pending is not None:
                    pending[s].wait()
                dim = CORE if step < 0 else orders[height][kind(height, s)][step]
                span = pl.ds(bases[s], size)
                copies.append(remote(bufs[s].at[span], bufs[s].at[span], dim))
                if step >= 0:
                    bases[s] = bases[s] - mine(dim) * size
            pending = copies
            size *= 2
        middle()
        for copy in pending:
            copy.wait()

    def apply_rows(index, height, bufs, lane):
        half = halves[height]
        for at in range(half):
            block = jnp.concatenate(
                [bufs[s][lane * half + perms[height][kind(height, s)][at]] for s in range(stripes)], axis=0
            )
            high, low = split(block)
            left_ref[0:BLK, at * BLK : (at + 1) * BLK] = high
            left_ref[BLK : 2 * BLK, at * BLK : (at + 1) * BLK] = low
        full = dot(left_ref[:, 0 : half * BLK], stacked[index][lane], 1)
        both = full[:BLK] + full[BLK:]
        rows = both.shape[1] // 2
        return both[:, :rows] + both[:, rows:]

    def apply_cols(index, height, bufs, vector, lane):
        half = halves[height]
        high, low = split(vector)
        left = jnp.concatenate(
            [jnp.concatenate([high, high], axis=1), jnp.concatenate([low, low], axis=1)], axis=0
        )
        for at in range(0, half, 2):
            full = dot(left, stacked[index][lane, :, at * BLK : (at + 2) * BLK], 0)
            both = full[:BLK] + full[BLK:]
            for step in range(2):
                for s in range(stripes):
                    bufs[s][lane * half + perms[height][kind(height, s)][at + step]] = both[
                        lows[s] : lows[s] + stripe_rows[s], step * BLK : (step + 1) * BLK
                    ]

    def gathered_rows(index, height, bufs, bases, size, depth):
        lane = lanes[height]
        parts = []
        gather_steps(
            height, bufs, bases, size, depth, lambda: parts.append(apply_rows(index, height, bufs, lane))
        )
        return parts[0] + apply_rows(index, height, bufs, 1 - lane)

    inverses = (0, 2, 4, 6)
    couplings = (1, 3, 5)
    starts = [sum(pivots[:h]) for h in range(HEIGHTS)]

    def right_side(height, part):
        low = (starts[height] + part * BLK) // 8
        return ordered[low : low + BLK // 8].reshape(BLK, -1).T

    def keep_solution(height, slots):
        for part in range(piece_of[height]):
            low = starts[height] + part * BLK
            sol[low : low + BLK, :] = own_block(whole_vec[height], slots, part).T

    slots = own_slots(0)
    for part in range(piece_of[0]):
        value = right_side(0, part)
        for s in range(stripes):
            partial[0][s][slots[s] + part] = value[lows[s] : lows[s] + stripe_rows[s]]
    solved[0][...] = gathered_rows(
        inverses[0], 0, partial[0], slots, piece_of[0], len(orders[0][0])
    )
    for height in range(1, HEIGHTS):
        vector = -solved[height - 1][...]
        bufs = partial[height]

        def fill(lane, height=height, vector=vector, bufs=bufs):
            apply_cols(couplings[height - 1], height, bufs, vector, lane)
            if lane is lanes[height]:
                value = right_side(height, 0)
                slots = own_slots(height)
                for s in range(stripes):
                    bufs[s][slots[s]] = bufs[s][slots[s]] + value[lows[s] : lows[s] + stripe_rows[s]]

        bases = reduce_steps(height, 2 * halves[height] - 2, fill)
        solved[height][...] = gathered_rows(
            inverses[height], height, whole_vec[height], bases, 2, len(orders[height][0]) - 1
        )
    target = solved[HEIGHTS - 1][...]
    for height in range(HEIGHTS - 1, -1, -1):
        bufs = partial[height]

        def fill(lane, height=height, vector=target, bufs=bufs):
            apply_cols(inverses[height], height, bufs, vector, lane)

        bases = reduce_steps(height, 2 * halves[height] if height > 0 else None, fill)
        keep_solution(height, own_slots(height))
        if height > 0:
            target = solved[height - 1][...] - gathered_rows(
                couplings[height - 1], height, whole_vec[height], bases, 2, len(orders[height][0]) - 1
            )

    exchange_rows(
        back_pack_idx, lambda i: sol[pl.ds(i, 1), :], returned, back_send, back_recv, lambda: None
    )
    finish_rows(returned, back_send, back_recv)
    unpack_rows(back_idx, returned, out_ref)


def solve(app_rhs, tables, weights, cap):
    leaves = lax.axis_size("leaf")
    fronts = lax.axis_size("front")
    peers = leaves * fronts
    front_bits = fronts.bit_length() - 1
    leaf_bits = leaves.bit_length() - 1
    rows, rhs_count = app_rhs.shape
    units = [unit * rhs_count // BLK for unit in STRIPE_UNITS]
    stripe_rows = tuple(8 * unit for unit in units)
    inverses = (weights[0], weights[2], weights[4], weights[6])
    sizes = tuple(w.shape[1] for w in inverses)
    pivots = tuple(w.shape[0] for w in inverses)
    blocks = [size // BLK for size in sizes]

    def stripe_buffers(count):
        return [pltpu.VMEM((count, height, BLK), jnp.float32) for height in stripe_rows]

    copies = 0
    for height in range(HEIGHTS):
        depth = len(group_dims(front_bits, height))
        copies += 2 * (depth + 1) if height == 0 else 2 * (2 * depth + 1)
    copies *= len(stripe_rows)
    scratch = [
        pltpu.VMEM((peers * cap, 1, rhs_count), jnp.float32),
        pltpu.VMEM((peers * cap, 1, rhs_count), jnp.float32),
        pltpu.VMEM((peers * cap, 1, rhs_count), jnp.float32),
        pltpu.VMEM((rows // 8, 8, rhs_count), jnp.float32),
        pltpu.VMEM((rows, rhs_count), jnp.float32),
        pltpu.VMEM((2, BLK, max(w.shape[1] for w in weights)), jnp.float32),
    ]
    scratch += [pltpu.VMEM((2, 2 * w.shape[0], w.shape[1] // 2), jnp.bfloat16) for w in weights]
    scratch += [pltpu.VMEM((2 * rhs_count, max(sizes) // 2), jnp.bfloat16)]
    scratch += [pltpu.VMEM((rhs_count, count), jnp.float32) for count in pivots]
    for count in blocks + [count + 2 for count in blocks] + blocks[1:]:
        scratch += stripe_buffers(count)
    scratch += [
        pltpu.SemaphoreType.DMA((2,)),
        pltpu.SemaphoreType.DMA((copies,)),
        pltpu.SemaphoreType.DMA((copies,)),
    ]
    scratch += [pltpu.SemaphoreType.DMA((peers - 1,)) for _ in range(4)]
    vmem = pl.BlockSpec(memory_space=pltpu.VMEM)
    smem = pl.BlockSpec(memory_space=pltpu.SMEM)
    out = pl.pallas_call(
        functools.partial(solve_kernel, leaf_bits, front_bits, stripe_rows, pivots, sizes, cap),
        out_shape=jax.ShapeDtypeStruct((rows // 8, 8, rhs_count), jnp.float32),
        in_specs=[vmem] + [smem] * 4 + [pl.BlockSpec(memory_space=pl.ANY)] * 7,
        out_specs=vmem,
        scratch_shapes=scratch,
        compiler_params=pltpu.CompilerParams(
            collective_id=0, has_side_effects=True, vmem_limit_bytes=66 * 1024 * 1000
        ),
    )(app_rhs.reshape(rows, 1, rhs_count), *tables, *weights)
    return out.reshape(rows, rhs_count)


def slots_of(owner, order, row_count, cap):
    block = owner // row_count
    before = (block[:, None] == block[None, :]) & (order[None, :] < order[:, None])
    return block * cap + jnp.sum(before.astype(jnp.int32), axis=1)


def rows_of(slots, slot_count):
    rows = jnp.arange(slots.shape[0], dtype=jnp.int32)
    same = jnp.arange(slot_count, dtype=jnp.int32)[:, None] == slots[None, :]
    return jnp.sum(jnp.where(same, rows[None, :], 0), axis=1)


def per_device(app_rhs, pivot_source, row_owner, *matrices):
    row_count = app_rhs.shape[0]
    peer_count = lax.axis_size("leaf") * lax.axis_size("front")
    mean_rows = row_count // (peer_count // 2)
    cap = mean_rows + max(1, mean_rows // 4)
    send_slots = slots_of(row_owner, jnp.arange(row_count, dtype=jnp.int32), row_count, cap)
    recv_slots = slots_of(pivot_source, pivot_source, row_count, cap)
    tables = (
        rows_of(send_slots, peer_count * cap),
        recv_slots,
        rows_of(recv_slots, peer_count * cap),
        send_slots,
    )
    return solve(app_rhs, tables, [w[0, 0] for w in matrices], cap)


def solution(mesh):
    rows = P(("leaf", "front"), None)
    flat = P(("leaf", "front"))
    blocks = P("leaf", "front", None, None)
    return jax.shard_map(
        per_device, mesh=mesh, in_specs=(rows, flat, flat) + (blocks,) * 7, out_specs=rows, check_vma=False
    )
```

```python
import functools

import jax
import jax.numpy as jnp
from jax import lax
from jax.experimental import pallas as pl
from jax.experimental.pallas import tpu as pltpu
from jax.sharding import PartitionSpec as P

BLK = 128
HEIGHTS = 4
CLASSES = 3
MESH = pl.DeviceIdType.MESH
CORE = ("front", 0)
GROUPS = 2
STRIPE_UNITS = (2, 2, 1, 1, 1, 1)


def bit_of(value, place):
    return lax.rem(lax.div(value, jnp.int32(2**place)), jnp.int32(2))


def flipped(value, mask, bits):
    out = jnp.int32(0)
    for place in range(bits):
        out = out + lax.rem(bit_of(value, place) + bit_of(mask, place), jnp.int32(2)) * 2**place
    return out


def group_dims(front_bits, height):
    return [("front", place) for place in range(1, front_bits)] + [("leaf", place) for place in range(height)]


def group_orders(front_bits, height):
    dims = group_dims(front_bits, height)
    turns = min(CLASSES, len(dims))
    head, rest = dims[:turns], dims[turns:]
    return [head[turn:] + head[:turn] + rest for turn in range(turns)]


def place_slot(place, height, order):
    slot = 0
    for axis, at in order:
        slot = slot * 2 + (place >> (at + height if axis == "front" else at) & 1)
    return slot


def place_lane(place):
    return bin(place).count("1") % 2


def split(value):
    high = value.astype(jnp.bfloat16)
    return high, (value - high.astype(jnp.float32)).astype(jnp.bfloat16)


def dot(left, right, right_axis):
    dims = (((1,), (right_axis,)), ((), ()))
    return lax.dot_general(left, right, dimension_numbers=dims, preferred_element_type=jnp.float32)


def solve_kernel(leaf_bits, front_bits, stripe_rows, pivots, sizes, cap, *refs):
    app_ref, pack_idx, order_idx, back_pack_idx, back_idx = refs[:5]
    weights_hbm = refs[5:12]
    out_ref = refs[12]
    packed, arrived, returned, ordered, sol, right_ref, done_ref = refs[13:20]
    near, far = refs[20:22]
    stacked = refs[22:29]
    left_ref = refs[29]
    solved = refs[30:34]
    pair_out, pair_in = refs[34:36]
    buffers = refs[36:-12]
    near_sems, far_send, far_recv, free_sem, pair_send, pair_recv = refs[-12:-6]
    send_sems, recv_sems, go_send, go_recv, back_send, back_recv = refs[-6:]
    stripes = len(stripe_rows)
    per_group = stripes // GROUPS
    width = sum(stripe_rows[:per_group])
    lows = [sum(stripe_rows[:s]) % width for s in range(stripes)]
    pos = 0

    def take(count):
        nonlocal pos
        pos += count
        return buffers[pos - count : pos]

    partial = [take(stripes) for _ in range(HEIGHTS)]
    recv = [take(stripes) for _ in range(HEIGHTS)]
    whole_vec = [partial[0]] + [take(stripes) for _ in range(HEIGHTS - 1)]

    leaf = lax.axis_index("leaf")
    front = lax.axis_index("front")
    fronts = 2**front_bits
    peers = 2 ** (front_bits + leaf_bits)
    here = {"leaf": leaf, "front": front}
    me = leaf * fronts + front

    def mine(dim):
        return bit_of(here[dim[0]], dim[1])

    core_flip = front + (1 - 2 * mine(CORE))

    def partner(dim):
        axis, place = dim
        if dim == CORE:
            return (leaf, core_flip)
        move = (1 - 2 * mine(dim)) * 2**place
        return (leaf + move, core_flip) if axis == "leaf" else (leaf, core_flip + move)

    def peer(step):
        turn = jnp.int32(peers - 1) - step
        return (
            flipped(leaf, lax.div(turn, jnp.int32(fronts)), leaf_bits),
            flipped(front, lax.rem(turn, jnp.int32(fronts)), front_bits),
        )

    piece_of = [pivots[h] // BLK for h in range(HEIGHTS)]
    halves = [size // BLK // 2 for size in sizes]
    orders = [group_orders(front_bits, h) for h in range(HEIGHTS)]
    lanes = []
    for height in range(HEIGHTS):
        total = jnp.int32(0)
        for place in range(front_bits):
            total = total + bit_of(front, place)
        for place in range(height):
            total = total + bit_of(leaf, place)
        lanes.append(lax.rem(total, jnp.int32(2)))

    def kind(height, stripe):
        return stripe % per_group % len(orders[height])

    places = []
    for height in range(HEIGHTS):
        table = {}
        for place in range(2 ** (front_bits + height)):
            if not place >> height & 1:
                table[place_slot(place, height, orders[height][0])] = place
        places.append(table)

    perms = []
    for height in range(HEIGHTS):
        table = [[0] * halves[height] for _ in orders[height]]
        for place in range(2 ** (front_bits + height)):
            canon = place_slot(place, height, orders[height][0])
            for k, order in enumerate(orders[height]):
                for part in range(piece_of[height]):
                    table[k][canon * piece_of[height] + part] = (
                        place_slot(place, height, order) * piece_of[height] + part
                    )
        perms.append(table)

    weight_heights = (0, 1, 1, 2, 2, 3, 3)
    pieces = []
    for index in range(7):
        for part in range(weights_hbm[index].shape[0] // BLK):
            pieces.append((index, part))

    def column(height, at, lane):
        piece = piece_of[height]
        place, rest = places[height][at // piece], at % piece
        core = lax.rem(lane + place_lane(place), jnp.int32(2))
        return pl.multiple_of((place * piece + rest) * BLK + core * (2**height * piece * BLK), BLK)

    def block_copies(number, lane):
        index, part = pieces[number]
        height = weight_heights[index]
        for at in range(halves[height]):
            yield at, weights_hbm[index].at[pl.ds(part * BLK, BLK), pl.ds(column(height, at, lane), BLK)]

    def start_near(number):
        for at, source in block_copies(number, lanes[weight_heights[pieces[number][0]]]):
            pltpu.make_async_copy(source, near.at[number % 2, at], near_sems.at[number % 2]).start()

    def far_copy(number, at, source):
        return pltpu.make_async_remote_copy(
            src_ref=source,
            dst_ref=at,
            send_sem=far_send.at[number % 2],
            recv_sem=far_recv.at[number % 2],
            device_id=(leaf, core_flip),
            device_id_type=MESH,
        )

    def start_far(number):
        for at, source in block_copies(number, 1 - lanes[weight_heights[pieces[number][0]]]):
            far_copy(number, far.at[number % 2, at], source).start()

    start_near(0)
    start_near(1)

    barrier = pltpu.get_barrier_semaphore()

    def greet(step, carry):
        pl.semaphore_signal(barrier, inc=1, device_id=peer(step), device_id_type=MESH)
        return carry

    lax.fori_loop(0, peers - 1, greet, 0)

    def pack_rows(index, source, target, base, where):
        for row in range(cap):
            target[base + row] = source(index[where + row])

    def send_to(step, source, target, sends, recvs):
        to_leaf, to_front = peer(step)
        there = to_leaf * fronts + to_front
        return pltpu.make_async_remote_copy(
            src_ref=source.at[pl.ds(there * cap, cap)],
            dst_ref=target.at[pl.ds(me * cap, cap)],
            send_sem=sends.at[0],
            recv_sem=recvs.at[0],
            device_id=(to_leaf, to_front),
            device_id_type=MESH,
        )

    def exchange_rows(index, source, target, sends, recvs, ready):
        def pack(step):
            to_leaf, to_front = peer(step)
            base = (to_leaf * fronts + to_front) * cap
            pack_rows(index, source, packed, base, base)

        if ready is not None:
            lax.fori_loop(0, peers - 1, lambda step, carry: (pack(step), carry)[1], 0)
            pack_rows(index, source, target, me * cap, me * cap)
            ready()

            def launch(step, carry):
                send_to(step, packed, target, sends, recvs).start()
                return carry

            lax.fori_loop(0, peers - 1, launch, 0)
            return

        pack(jnp.int32(0))

        def body(step, carry):
            pack(step)
            send_to(step - 1, packed, target, sends, recvs).start()
            return carry

        lax.fori_loop(1, peers - 1, body, 0)
        pack_rows(index, source, target, me * cap, me * cap)
        send_to(jnp.int32(peers - 2), packed, target, sends, recvs).start()

    def finish_rows(target, sends, recvs):
        for ref, sem in ((packed, sends), (target, recvs)):
            span = ref.at[pl.ds(0, (peers - 1) * cap)]
            pltpu.make_async_copy(span, span, sem.at[0]).wait()

    def unpack_rows(index, source, target):
        def body(group, carry):
            for row in range(8):
                target[group, pl.ds(row, 1), :] = source[index[group * 8 + row]]
            return carry

        lax.fori_loop(0, target.shape[0], body, 0, unroll=2)

    exchange_rows(
        pack_idx,
        lambda i: app_ref[i],
        arrived,
        go_send,
        go_recv,
        lambda: pl.semaphore_wait(barrier, peers - 1),
    )
    start_far(0)
    start_far(1)

    for number, (index, part) in enumerate(pieces):
        rows = weights_hbm[index].shape[0]
        half = halves[weight_heights[index]]
        slot = number % 2
        here_all, there_all = near.at[slot, pl.ds(0, half)], far.at[slot, pl.ds(0, half)]
        pltpu.make_async_copy(here_all, here_all, near_sems.at[slot]).wait()
        far_copy(number, there_all, there_all).wait()

        def convert(group, carry, index=index, part=part, rows=rows, half=half, slot=slot):
            span = pl.ds(pl.multiple_of(group * 16, 16), 16)
            for side, source in enumerate((near, far)):
                for at in range(half):
                    for level, value in enumerate(split(source[slot, at, span, :])):
                        start = (2 * side + level) * rows + part * BLK + group * 16
                        stacked[index][pl.ds(pl.multiple_of(start, 16), 16), pl.ds(at * BLK, BLK)] = value
            return carry

        lax.fori_loop(0, BLK // 16, convert, 0)
        if number + 2 < len(pieces):
            pl.semaphore_signal(free_sem, inc=1, device_id=(leaf, core_flip), device_id_type=MESH)
            start_near(number + 2)
            pl.semaphore_wait(free_sem, 1)
            start_far(number + 2)

    finish_rows(arrived, go_send, go_recv)
    unpack_rows(order_idx, arrived, ordered)

    all_dims = [CORE] + group_dims(front_bits, leaf_bits)

    def remote(source, target, dim, stripe, role):
        if role < 2:
            role = role * len(all_dims) + all_dims.index(dim)
        else:
            role = role - 2 + 2 * len(all_dims)
        index = role * stripes + stripe
        copy = pltpu.make_async_remote_copy(
            src_ref=source,
            dst_ref=target,
            send_sem=send_sems.at[stripe],
            recv_sem=recv_sems.at[index],
            device_id=partner(dim),
            device_id_type=MESH,
        )
        copy.start()
        return copy

    def members(group):
        return range(group * per_group, (group + 1) * per_group)

    def own_slot(height, stripe):
        slot = jnp.int32(0)
        for dim in orders[height][kind(height, stripe)]:
            slot = slot * 2 + mine(dim)
        return slot * piece_of[height]

    def reduce_steps(group, height, swap_at, bases):
        bufs, recvs, result = partial[height], recv[height], whole_vec[height]
        depth = len(orders[height][0])
        whole, prior, offset = halves[height], 0, 0
        pending = {}
        for step in range(depth + 1):
            full = swap_at is not None and step == depth - 1
            size = whole if full else whole // 2
            if full:
                offset = swap_at
            if step > 0:
                yield
            for s in members(group):
                if step > 0:
                    pending[s].wait()
                    keep = pl.ds(bases[s], whole)
                    (result if step == depth else bufs)[s][keep] = bufs[s][keep] + recvs[s][pl.ds(prior, whole)]
                if step < depth:
                    dim = orders[height][kind(height, s)][step]
                    away, role = bases[s], 0
                    if full:
                        role = 2 * height + (swap_at == halves[height])
                    else:
                        away = bases[s] + (1 - mine(dim)) * size
                        bases[s] = bases[s] + mine(dim) * size
                    pending[s] = remote(
                        bufs[s].at[pl.ds(away, size)], recvs[s].at[pl.ds(offset, size)], dim, s, role
                    )
            prior, whole = offset, size
            offset += size

    def gather_steps(group, height, bases, size, depth):
        bufs = whole_vec[height]
        pending = {}
        for step in range(depth - 1, -1, -1):
            for s in members(group):
                if pending.get(s) is not None:
                    pending[s].wait()
                dim = orders[height][kind(height, s)][step]
                span = pl.ds(bases[s], size)
                pending[s] = remote(bufs[s].at[span], bufs[s].at[span], dim, s, 1)
                bases[s] = bases[s] - mine(dim) * size
            size *= 2
            yield
        for s in members(group):
            pending[s].wait()

    turns = [0] * GROUPS

    def apply_rows(group, index, height, finish):
        bufs, half = whole_vec[height], halves[height]
        for at in range(half):
            block = jnp.concatenate(
                [bufs[s][perms[height][kind(height, s)][at]] for s in members(group)], axis=0
            )
            high, low = split(block)
            left_ref[0:width, at * BLK : (at + 1) * BLK] = high
            left_ref[width : 2 * width, at * BLK : (at + 1) * BLK] = low
        full = dot(left_ref[:, 0 : half * BLK], stacked[index][...], 1)
        both = full[:width] + full[width:]
        rows = both.shape[1] // 4
        turn = turns[group] % 2
        turns[group] += 1
        for side in range(2):
            low = 2 * side * rows
            pair_out[group, side, :, 0:rows] = both[:, low : low + rows] + both[:, low + rows : low + 2 * rows]
        copy = pltpu.make_async_remote_copy(
            src_ref=pair_out.at[group, :, :, pl.ds(0, rows)],
            dst_ref=pair_in.at[group, turn, :, :, pl.ds(0, rows)],
            send_sem=pair_send.at[group],
            recv_sem=pair_recv.at[2 * group + turn],
            device_id=(leaf, core_flip),
            device_id_type=MESH,
        )
        copy.start()
        yield
        copy.wait()
        finish(
            jnp.concatenate(
                [pair_out[group, side, :, 0:rows] + pair_in[group, turn, 1 - side, :, 0:rows] for side in range(2)],
                axis=1,
            )
        )

    def apply_cols(group, index, height, vector):
        bufs, half = partial[height], halves[height]
        rows = vector.shape[1] // 2
        sides = []
        for part in split(vector):
            near_part, far_part = part[:, :rows], part[:, rows:]
            sides.append(jnp.concatenate([near_part, near_part, far_part, far_part], axis=1))
        left = jnp.concatenate(sides, axis=0)
        for at in range(0, half, 2):
            full = dot(left, stacked[index][:, at * BLK : (at + 2) * BLK], 0)
            both = full[:width] + full[width:]
            for step in range(2):
                for s in members(group):
                    bufs[s][perms[height][kind(height, s)][at + step]] = both[
                        lows[s] : lows[s] + stripe_rows[s], step * BLK : (step + 1) * BLK
                    ]

    inverses = (0, 2, 4, 6)
    couplings = (1, 3, 5)
    starts = [sum(pivots[:h]) // BLK for h in range(HEIGHTS)]
    for part in range(right_ref.shape[0]):
        low = part * BLK // 8
        right_ref[part] = ordered[low : low + BLK // 8].reshape(BLK, -1).T

    def chain(group):
        def keep_value(height):
            def keep(value):
                solved[height][group] = value

            return keep

        def own_right(height, part, s):
            low = group * width + lows[s]
            return right_ref[starts[height] + part, low : low + stripe_rows[s]]

        bases = {s: own_slot(0, s) for s in members(group)}
        for part in range(piece_of[0]):
            for s in members(group):
                partial[0][s][bases[s] + part] = own_right(0, part, s)
        yield from gather_steps(group, 0, bases, piece_of[0], len(orders[0][0]))
        yield from apply_rows(group, inverses[0], 0, keep_value(0))
        for height in range(1, HEIGHTS):
            apply_cols(group, couplings[height - 1], height, -solved[height - 1][group])
            for s in members(group):
                spot, slot = partial[height][s], own_slot(height, s)
                spot[slot] = spot[slot] + own_right(height, 0, s)
            bases = {s: jnp.int32(0) for s in members(group)}
            yield from reduce_steps(group, height, halves[height] - 2, bases)
            yield from gather_steps(group, height, bases, 2, len(orders[height][0]) - 1)
            yield from apply_rows(group, inverses[height], height, keep_value(height))
        target = [solved[HEIGHTS - 1][group]]
        for height in range(HEIGHTS - 1, -1, -1):
            apply_cols(group, inverses[height], height, target.pop())
            bases = {s: jnp.int32(0) for s in members(group)}
            yield from reduce_steps(group, height, halves[height] if height > 0 else None, bases)
            for part in range(piece_of[height]):
                for s in members(group):
                    low = group * width + lows[s]
                    done_ref[starts[height] + part, low : low + stripe_rows[s]] = whole_vec[height][s][
                        own_slot(height, s) + part
                    ]
            if height > 0:
                yield from gather_steps(group, height, bases, 2, len(orders[height][0]) - 1)
                yield from apply_rows(
                    group,
                    couplings[height - 1],
                    height,
                    lambda value: target.append(solved[height - 1][group] - value),
                )

    chains = [chain(group) for group in range(GROUPS)]
    while chains:
        for running in list(chains):
            if next(running, chains) is chains:
                chains.remove(running)
    for part in range(done_ref.shape[0]):
        sol[part * BLK : (part + 1) * BLK, :] = done_ref[part].T

    exchange_rows(
        back_pack_idx, lambda i: sol[pl.ds(i, 1), :], returned, back_send, back_recv, None
    )
    finish_rows(returned, back_send, back_recv)
    unpack_rows(back_idx, returned, out_ref)


def solve(app_rhs, tables, weights, cap):
    leaves = lax.axis_size("leaf")
    fronts = lax.axis_size("front")
    peers = leaves * fronts
    front_bits = fronts.bit_length() - 1
    leaf_bits = leaves.bit_length() - 1
    rows, rhs_count = app_rhs.shape
    units = [unit * rhs_count // BLK for unit in STRIPE_UNITS * GROUPS]
    width = rhs_count // GROUPS
    stripe_rows = tuple(8 * unit for unit in units)
    inverses = (weights[0], weights[2], weights[4], weights[6])
    sizes = tuple(w.shape[1] for w in inverses)
    pivots = tuple(w.shape[0] for w in inverses)
    blocks = [size // BLK for size in sizes]

    def stripe_buffers(count):
        return [pltpu.VMEM((count, height, BLK), jnp.float32) for height in stripe_rows]

    copies = (2 * (1 + len(group_dims(front_bits, leaf_bits))) + 2 * (HEIGHTS - 1)) * len(stripe_rows)
    scratch = [
        pltpu.VMEM((peers * cap, 1, rhs_count), jnp.float32),
        pltpu.VMEM((peers * cap, 1, rhs_count), jnp.float32),
        pltpu.VMEM((peers * cap, 1, rhs_count), jnp.float32),
        pltpu.VMEM((rows // 8, 8, rhs_count), jnp.float32),
        pltpu.VMEM((rows, rhs_count), jnp.float32),
        pltpu.VMEM((rows // BLK, rhs_count, BLK), jnp.float32),
        pltpu.VMEM((rows // BLK, rhs_count, BLK), jnp.float32),
        pltpu.VMEM((2, max(blocks) // 2, BLK, BLK), jnp.float32),
        pltpu.VMEM((2, max(blocks) // 2, BLK, BLK), jnp.float32),
    ]
    scratch += [pltpu.VMEM((4 * w.shape[0], w.shape[1] // 2), jnp.bfloat16) for w in weights]
    scratch += [pltpu.VMEM((2 * width, max(sizes) // 2), jnp.bfloat16)]
    scratch += [pltpu.VMEM((GROUPS, width, 2 * count), jnp.float32) for count in pivots]
    scratch += [
        pltpu.VMEM((GROUPS, 2, width, max(pivots)), jnp.float32),
        pltpu.VMEM((GROUPS, 2, 2, width, max(pivots)), jnp.float32),
    ]
    lane_blocks = [count // 2 for count in blocks]
    for count in lane_blocks + [count + 2 for count in lane_blocks] + lane_blocks[1:]:
        scratch += stripe_buffers(count)
    scratch += [pltpu.SemaphoreType.DMA((2,)) for _ in range(3)]
    scratch += [pltpu.SemaphoreType.REGULAR]
    scratch += [pltpu.SemaphoreType.DMA((count,)) for count in (GROUPS, 2 * GROUPS)]
    scratch += [pltpu.SemaphoreType.DMA((count,)) for count in (len(stripe_rows), copies)]
    scratch += [pltpu.SemaphoreType.DMA((1,)) for _ in range(4)]
    vmem = pl.BlockSpec(memory_space=pltpu.VMEM)
    smem = pl.BlockSpec(memory_space=pltpu.SMEM)
    out = pl.pallas_call(
        functools.partial(solve_kernel, leaf_bits, front_bits, stripe_rows, pivots, sizes, cap),
        out_shape=jax.ShapeDtypeStruct((rows // 8, 8, rhs_count), jnp.float32),
        in_specs=[vmem] + [smem] * 4 + [pl.BlockSpec(memory_space=pl.ANY)] * 7,
        out_specs=vmem,
        scratch_shapes=scratch,
        compiler_params=pltpu.CompilerParams(
            collective_id=0, has_side_effects=True, vmem_limit_bytes=66 * 1024 * 1000
        ),
    )(app_rhs.reshape(rows, 1, rhs_count), *tables, *weights)
    return out.reshape(rows, rhs_count)


def slots_of(owner, order, row_count, cap):
    block = owner // row_count
    before = (block[:, None] == block[None, :]) & (order[None, :] < order[:, None])
    return block * cap + jnp.sum(before.astype(jnp.int32), axis=1)


def rows_of(slots, slot_count):
    rows = jnp.arange(slots.shape[0], dtype=jnp.int32)
    same = jnp.arange(slot_count, dtype=jnp.int32)[:, None] == slots[None, :]
    return jnp.sum(jnp.where(same, rows[None, :], 0), axis=1)


def per_device(app_rhs, pivot_source, row_owner, *matrices):
    row_count = app_rhs.shape[0]
    peer_count = lax.axis_size("leaf") * lax.axis_size("front")
    mean_rows = row_count // (peer_count // 2)
    cap = mean_rows + max(1, mean_rows // 4)
    send_slots = slots_of(row_owner, jnp.arange(row_count, dtype=jnp.int32), row_count, cap)
    recv_slots = slots_of(pivot_source, pivot_source, row_count, cap)
    tables = (
        rows_of(send_slots, peer_count * cap),
        recv_slots,
        rows_of(recv_slots, peer_count * cap),
        send_slots,
    )
    return solve(app_rhs, tables, [w[0, 0] for w in matrices], cap)


def solution(mesh):
    rows = P(("leaf", "front"), None)
    flat = P(("leaf", "front"))
    blocks = P("leaf", "front", None, None)
    return jax.shard_map(
        per_device, mesh=mesh, in_specs=(rows, flat, flat) + (blocks,) * 7, out_specs=rows, check_vma=False
    )
```

```python
import functools

import jax
import jax.numpy as jnp
from jax import lax
from jax.experimental import pallas as pl
from jax.experimental.pallas import tpu as pltpu
from jax.sharding import PartitionSpec as P

BLK = 128
HEIGHTS = 4
CLASSES = 3
MESH = pl.DeviceIdType.MESH
CORE = ("front", 0)
GROUPS = 2
STRIPE_UNITS = (2, 2, 1, 1, 1, 1)


def bit_of(value, place):
    return lax.rem(lax.div(value, jnp.int32(2**place)), jnp.int32(2))


def flipped(value, mask, bits):
    out = jnp.int32(0)
    for place in range(bits):
        out = out + lax.rem(bit_of(value, place) + bit_of(mask, place), jnp.int32(2)) * 2**place
    return out


def group_dims(front_bits, height):
    return [("front", place) for place in range(1, front_bits)] + [("leaf", place) for place in range(height)]


def group_orders(front_bits, height):
    dims = group_dims(front_bits, height)
    turns = min(CLASSES, len(dims))
    head, rest = dims[:turns], dims[turns:]
    return [head[turn:] + head[:turn] + rest for turn in range(turns)]


def swap_steps(height):
    return (0, 2, 2, 1)[height]


def kept_blocks(front_bits, height, half):
    return half >> (len(group_dims(front_bits, height)) - swap_steps(height))


def place_slot(place, height, order):
    slot = 0
    for axis, at in order:
        slot = slot * 2 + (place >> (at + height if axis == "front" else at) & 1)
    return slot


def place_lane(place):
    return bin(place).count("1") % 2


def split(value):
    high = value.astype(jnp.bfloat16)
    return high, (value - high.astype(jnp.float32)).astype(jnp.bfloat16)


def dot(left, right, right_axis):
    dims = (((1,), (right_axis,)), ((), ()))
    return lax.dot_general(left, right, dimension_numbers=dims, preferred_element_type=jnp.float32)


def solve_kernel(leaf_bits, front_bits, stripe_rows, pivots, sizes, cap, *refs):
    app_ref, pack_idx, order_idx, back_pack_idx, back_idx = refs[:5]
    weights_hbm = refs[5:12]
    out_ref = refs[12]
    packed, arrived, returned, ordered, sol, right_ref, done_ref = refs[13:20]
    near, far = refs[20:22]
    stacked = refs[22:29]
    left_ref = refs[29]
    solved = refs[30:34]
    pair_out, pair_in = refs[34:36]
    buffers = refs[36:-12]
    near_sems, far_send, far_recv, free_sem, pair_send, pair_recv = refs[-12:-6]
    send_sems, recv_sems, go_send, go_recv, back_send, back_recv = refs[-6:]
    stripes = len(stripe_rows)
    per_group = stripes // GROUPS
    width = sum(stripe_rows[:per_group])
    lows = [sum(stripe_rows[:s]) % width for s in range(stripes)]
    pos = 0

    def take(count):
        nonlocal pos
        pos += count
        return buffers[pos - count : pos]

    partial = [take(stripes) for _ in range(HEIGHTS)]
    recv = [take(stripes) for _ in range(HEIGHTS)]
    whole_vec = [partial[0]] + [take(stripes) for _ in range(HEIGHTS - 1)]

    leaf = lax.axis_index("leaf")
    front = lax.axis_index("front")
    fronts = 2**front_bits
    peers = 2 ** (front_bits + leaf_bits)
    here = {"leaf": leaf, "front": front}
    me = leaf * fronts + front

    def mine(dim):
        return bit_of(here[dim[0]], dim[1])

    core_flip = front + (1 - 2 * mine(CORE))

    def partner(dim):
        axis, place = dim
        if dim == CORE:
            return (leaf, core_flip)
        move = (1 - 2 * mine(dim)) * 2**place
        return (leaf + move, core_flip) if axis == "leaf" else (leaf, core_flip + move)

    def peer(step):
        turn = jnp.int32(peers - 1) - step
        return (
            flipped(leaf, lax.div(turn, jnp.int32(fronts)), leaf_bits),
            flipped(front, lax.rem(turn, jnp.int32(fronts)), front_bits),
        )

    piece_of = [pivots[h] // BLK for h in range(HEIGHTS)]
    halves = [size // BLK // 2 for size in sizes]
    orders = [group_orders(front_bits, h) for h in range(HEIGHTS)]
    lanes = []
    for height in range(HEIGHTS):
        total = jnp.int32(0)
        for place in range(front_bits):
            total = total + bit_of(front, place)
        for place in range(height):
            total = total + bit_of(leaf, place)
        lanes.append(lax.rem(total, jnp.int32(2)))

    def kind(height, stripe):
        return stripe % per_group % len(orders[height])

    places = []
    for height in range(HEIGHTS):
        table = {}
        for place in range(2 ** (front_bits + height)):
            if not place >> height & 1:
                table[place_slot(place, height, orders[height][0])] = place
        places.append(table)

    perms = []
    for height in range(HEIGHTS):
        table = [[0] * halves[height] for _ in orders[height]]
        for place in range(2 ** (front_bits + height)):
            canon = place_slot(place, height, orders[height][0])
            for k, order in enumerate(orders[height]):
                for part in range(piece_of[height]):
                    table[k][canon * piece_of[height] + part] = (
                        place_slot(place, height, order) * piece_of[height] + part
                    )
        perms.append(table)

    weight_heights = (0, 1, 1, 2, 2, 3, 3)
    pieces = []
    for index in range(7):
        for part in range(weights_hbm[index].shape[0] // BLK):
            pieces.append((index, part))

    def column(height, at, lane):
        piece = piece_of[height]
        place, rest = places[height][at // piece], at % piece
        core = lax.rem(lane + place_lane(place), jnp.int32(2))
        return pl.multiple_of((place * piece + rest) * BLK + core * (2**height * piece * BLK), BLK)

    def block_copies(number, lane):
        index, part = pieces[number]
        height = weight_heights[index]
        for at in range(halves[height]):
            yield at, weights_hbm[index].at[pl.ds(part * BLK, BLK), pl.ds(column(height, at, lane), BLK)]

    def start_near(number):
        for at, source in block_copies(number, lanes[weight_heights[pieces[number][0]]]):
            pltpu.make_async_copy(source, near.at[number % 2, at], near_sems.at[number % 2]).start()

    def far_copy(number, at, source):
        return pltpu.make_async_remote_copy(
            src_ref=source,
            dst_ref=at,
            send_sem=far_send.at[number % 2],
            recv_sem=far_recv.at[number % 2],
            device_id=(leaf, core_flip),
            device_id_type=MESH,
        )

    def start_far(number):
        for at, source in block_copies(number, 1 - lanes[weight_heights[pieces[number][0]]]):
            far_copy(number, far.at[number % 2, at], source).start()

    start_near(0)
    start_near(1)

    barrier = pltpu.get_barrier_semaphore()

    def greet(step):
        pl.semaphore_signal(barrier, inc=1, device_id=peer(step), device_id_type=MESH)


    def pack_rows(index, source, target, base, where):
        for row in range(cap):
            target[base + row] = source(index[where + row])

    def send_to(step, source, target, sends, recvs):
        to_leaf, to_front = peer(step)
        there = to_leaf * fronts + to_front
        return pltpu.make_async_remote_copy(
            src_ref=source.at[pl.ds(there * cap, cap)],
            dst_ref=target.at[pl.ds(me * cap, cap)],
            send_sem=sends.at[0],
            recv_sem=recvs.at[0],
            device_id=(to_leaf, to_front),
            device_id_type=MESH,
        )

    def exchange_rows(index, source, target, sends, recvs, ready):
        def pack(step):
            to_leaf, to_front = peer(step)
            base = (to_leaf * fronts + to_front) * cap
            pack_rows(index, source, packed, base, base)

        if ready is not None:

            def meet(step, carry):
                greet(step)
                pack(step)
                return carry

            lax.fori_loop(0, peers - 1, meet, 0)
            pack_rows(index, source, target, me * cap, me * cap)
            ready()

            def launch(step, carry):
                send_to(step, packed, target, sends, recvs).start()
                return carry

            lax.fori_loop(0, peers - 1, launch, 0)
            return

        pack(jnp.int32(0))

        def body(step, carry):
            pack(step)
            send_to(step - 1, packed, target, sends, recvs).start()
            return carry

        lax.fori_loop(1, peers - 1, body, 0)
        pack_rows(index, source, target, me * cap, me * cap)
        send_to(jnp.int32(peers - 2), packed, target, sends, recvs).start()

    def finish_rows(target, sends, recvs):
        for ref, sem in ((packed, sends), (target, recvs)):
            span = ref.at[pl.ds(0, (peers - 1) * cap)]
            pltpu.make_async_copy(span, span, sem.at[0]).wait()

    def unpack_rows(index, source, target):
        def body(group, carry):
            for row in range(8):
                target[group, pl.ds(row, 1), :] = source[index[group * 8 + row]]
            return carry

        lax.fori_loop(0, target.shape[0], body, 0, unroll=2)

    exchange_rows(
        pack_idx,
        lambda i: app_ref[i],
        arrived,
        go_send,
        go_recv,
        lambda: pl.semaphore_wait(barrier, peers - 1),
    )
    start_far(0)
    start_far(1)

    for number, (index, part) in enumerate(pieces):
        rows = weights_hbm[index].shape[0]
        half = halves[weight_heights[index]]
        slot = number % 2
        here_all, there_all = near.at[slot, pl.ds(0, half)], far.at[slot, pl.ds(0, half)]
        pltpu.make_async_copy(here_all, here_all, near_sems.at[slot]).wait()
        far_copy(number, there_all, there_all).wait()

        def convert(group, carry, index=index, part=part, rows=rows, half=half, slot=slot):
            span = pl.ds(pl.multiple_of(group * 16, 16), 16)
            for side, source in enumerate((near, far)):
                for at in range(half):
                    for level, value in enumerate(split(source[slot, at, span, :])):
                        start = (2 * side + level) * rows + part * BLK + group * 16
                        stacked[index][pl.ds(pl.multiple_of(start, 16), 16), pl.ds(at * BLK, BLK)] = value
            return carry

        lax.fori_loop(0, BLK // 16, convert, 0)
        if number + 2 < len(pieces):
            pl.semaphore_signal(free_sem, inc=1, device_id=(leaf, core_flip), device_id_type=MESH)
            start_near(number + 2)
            pl.semaphore_wait(free_sem, 1)
            start_far(number + 2)

    finish_rows(arrived, go_send, go_recv)
    unpack_rows(order_idx, arrived, ordered)

    all_dims = group_dims(front_bits, leaf_bits)

    def remote(source, target, dim, stripe, role):
        if role < 2:
            role = role * len(all_dims) + all_dims.index(dim)
        else:
            role = role - 2 + 2 * len(all_dims)
        index = role * stripes + stripe
        copy = pltpu.make_async_remote_copy(
            src_ref=source,
            dst_ref=target,
            send_sem=send_sems.at[stripe],
            recv_sem=recv_sems.at[index],
            device_id=partner(dim),
            device_id_type=MESH,
        )
        copy.start()
        return copy

    def members(group):
        return range(group * per_group, (group + 1) * per_group)

    def own_slot(height, stripe):
        slot = jnp.int32(0)
        for dim in orders[height][kind(height, stripe)]:
            slot = slot * 2 + mine(dim)
        return slot * piece_of[height]

    def reduce_steps(group, height, way, bases):
        bufs, recvs, result = partial[height], recv[height], whole_vec[height]
        depth = len(orders[height][0])
        whole, prior, offset = halves[height], 0, 0
        swaps = swap_steps(height)
        kept = kept_blocks(front_bits, height, whole)
        pending = {}
        for step in range(depth + 1):
            full = depth - swaps <= step
            size = whole if full else whole // 2
            number = way * swaps + step - depth + swaps
            if full:
                offset = halves[height] - kept + number * kept
            if step > 0:
                yield
            for s in members(group):
                if step > 0:
                    pending[s].wait()
                    keep = pl.ds(bases[s], whole)
                    (result if step == depth else bufs)[s][keep] = bufs[s][keep] + recvs[s][pl.ds(prior, whole)]
                if step < depth:
                    dim = orders[height][kind(height, s)][step]
                    away, role = bases[s], 0
                    if full:
                        role = 2 * height + (way if height == HEIGHTS - 1 else number % swaps)
                    else:
                        away = bases[s] + (1 - mine(dim)) * size
                        bases[s] = bases[s] + mine(dim) * size
                    pending[s] = remote(
                        bufs[s].at[pl.ds(away, size)], recvs[s].at[pl.ds(offset, size)], dim, s, role
                    )
            prior, whole = offset, size
            offset += size

    def gather_steps(group, height, bases, size, depth):
        bufs = whole_vec[height]
        pending = {}
        for step in range(depth - 1, -1, -1):
            for s in members(group):
                if pending.get(s) is not None:
                    pending[s].wait()
                dim = orders[height][kind(height, s)][step]
                span = pl.ds(bases[s], size)
                pending[s] = remote(bufs[s].at[span], bufs[s].at[span], dim, s, 1)
                bases[s] = bases[s] - mine(dim) * size
            size *= 2
            yield
        for copy in pending.values():
            copy.wait()

    def spread_steps(group, height, bases):
        kept = kept_blocks(front_bits, height, halves[height])
        return gather_steps(group, height, bases, kept, len(orders[height][0]) - swap_steps(height))

    turns = [0] * GROUPS

    def apply_rows(group, index, height, finish):
        bufs, half = whole_vec[height], halves[height]
        for at in range(half):
            block = jnp.concatenate(
                [bufs[s][perms[height][kind(height, s)][at]] for s in members(group)], axis=0
            )
            high, low = split(block)
            left_ref[0:width, at * BLK : (at + 1) * BLK] = high
            left_ref[width : 2 * width, at * BLK : (at + 1) * BLK] = low
        full = dot(left_ref[:, 0 : half * BLK], stacked[index][...], 1)
        both = full[:width] + full[width:]
        rows = both.shape[1] // 4
        turn = turns[group] % 2
        turns[group] += 1
        for side in range(2):
            low = 2 * side * rows
            pair_out[group, side, :, 0:rows] = both[:, low : low + rows] + both[:, low + rows : low + 2 * rows]
        copy = pltpu.make_async_remote_copy(
            src_ref=pair_out.at[group, :, :, pl.ds(0, rows)],
            dst_ref=pair_in.at[group, turn, :, :, pl.ds(0, rows)],
            send_sem=pair_send.at[group],
            recv_sem=pair_recv.at[2 * group + turn],
            device_id=(leaf, core_flip),
            device_id_type=MESH,
        )
        copy.start()
        yield
        copy.wait()
        finish(
            jnp.concatenate(
                [pair_out[group, side, :, 0:rows] + pair_in[group, turn, 1 - side, :, 0:rows] for side in range(2)],
                axis=1,
            )
        )

    def apply_cols(group, index, height, vector):
        bufs, half = partial[height], halves[height]
        rows = vector.shape[1] // 2
        sides = []
        for part in split(vector):
            near_part, far_part = part[:, :rows], part[:, rows:]
            sides.append(jnp.concatenate([near_part, near_part, far_part, far_part], axis=1))
        left = jnp.concatenate(sides, axis=0)
        for at in range(0, half, 2):
            full = dot(left, stacked[index][:, at * BLK : (at + 2) * BLK], 0)
            both = full[:width] + full[width:]
            for step in range(2):
                for s in members(group):
                    bufs[s][perms[height][kind(height, s)][at + step]] = both[
                        lows[s] : lows[s] + stripe_rows[s], step * BLK : (step + 1) * BLK
                    ]

    inverses = (0, 2, 4, 6)
    couplings = (1, 3, 5)
    starts = [sum(pivots[:h]) // BLK for h in range(HEIGHTS)]
    for part in range(right_ref.shape[0]):
        low = part * BLK // 8
        right_ref[part] = ordered[low : low + BLK // 8].reshape(BLK, -1).T

    def chain(group):
        def keep_value(height):
            def keep(value):
                solved[height][group] = value

            return keep

        def own_right(height, part, s):
            low = group * width + lows[s]
            return right_ref[starts[height] + part, low : low + stripe_rows[s]]

        bases = {s: own_slot(0, s) for s in members(group)}
        for part in range(piece_of[0]):
            for s in members(group):
                partial[0][s][bases[s] + part] = own_right(0, part, s)
        yield from gather_steps(group, 0, bases, piece_of[0], len(orders[0][0]))
        yield from apply_rows(group, inverses[0], 0, keep_value(0))
        for height in range(1, HEIGHTS):
            apply_cols(group, couplings[height - 1], height, -solved[height - 1][group])
            for s in members(group):
                spot, slot = partial[height][s], own_slot(height, s)
                spot[slot] = spot[slot] + own_right(height, 0, s)
            bases = dict.fromkeys(members(group), 0)
            yield from reduce_steps(group, height, 0, bases)
            yield from spread_steps(group, height, bases)
            yield from apply_rows(group, inverses[height], height, keep_value(height))
        target = [solved[HEIGHTS - 1][group]]
        for height in range(HEIGHTS - 1, -1, -1):
            apply_cols(group, inverses[height], height, target.pop())
            bases = dict.fromkeys(members(group), 0)
            yield from reduce_steps(group, height, 1, bases)
            for part in range(piece_of[height]):
                for s in members(group):
                    low = group * width + lows[s]
                    done_ref[starts[height] + part, low : low + stripe_rows[s]] = whole_vec[height][s][
                        own_slot(height, s) + part
                    ]
            if height > 0:
                yield from spread_steps(group, height, bases)
                yield from apply_rows(
                    group,
                    couplings[height - 1],
                    height,
                    lambda value: target.append(solved[height - 1][group] - value),
                )

    chains = [chain(group) for group in range(GROUPS)]
    while chains:
        for running in list(chains):
            if next(running, chains) is chains:
                chains.remove(running)
    for part in range(done_ref.shape[0]):
        sol[part * BLK : (part + 1) * BLK, :] = done_ref[part].T

    exchange_rows(
        back_pack_idx, lambda i: sol[pl.ds(i, 1), :], returned, back_send, back_recv, None
    )
    finish_rows(returned, back_send, back_recv)
    unpack_rows(back_idx, returned, out_ref)


def solve(app_rhs, tables, weights, cap):
    leaves = lax.axis_size("leaf")
    fronts = lax.axis_size("front")
    peers = leaves * fronts
    front_bits = fronts.bit_length() - 1
    leaf_bits = leaves.bit_length() - 1
    rows, rhs_count = app_rhs.shape
    units = [unit * rhs_count // BLK for unit in STRIPE_UNITS * GROUPS]
    width = rhs_count // GROUPS
    stripe_rows = tuple(8 * unit for unit in units)
    inverses = (weights[0], weights[2], weights[4], weights[6])
    sizes = tuple(w.shape[1] for w in inverses)
    pivots = tuple(w.shape[0] for w in inverses)
    blocks = [size // BLK for size in sizes]

    def stripe_buffers(count):
        return [pltpu.VMEM((count, height, BLK), jnp.float32) for height in stripe_rows]

    roles = 2 * len(group_dims(front_bits, leaf_bits)) + 2 * (HEIGHTS - 1)
    scratch = [
        pltpu.VMEM((peers * cap, 1, rhs_count), jnp.float32),
        pltpu.VMEM((peers * cap, 1, rhs_count), jnp.float32),
        pltpu.VMEM((peers * cap, 1, rhs_count), jnp.float32),
        pltpu.VMEM((rows // 8, 8, rhs_count), jnp.float32),
        pltpu.VMEM((rows, rhs_count), jnp.float32),
        pltpu.VMEM((rows // BLK, rhs_count, BLK), jnp.float32),
        pltpu.VMEM((rows // BLK, rhs_count, BLK), jnp.float32),
        pltpu.VMEM((2, max(blocks) // 2, BLK, BLK), jnp.float32),
        pltpu.VMEM((2, max(blocks) // 2, BLK, BLK), jnp.float32),
    ]
    scratch += [pltpu.VMEM((4 * w.shape[0], w.shape[1] // 2), jnp.bfloat16) for w in weights]
    scratch += [pltpu.VMEM((2 * width, max(sizes) // 2), jnp.bfloat16)]
    scratch += [pltpu.VMEM((GROUPS, width, 2 * count), jnp.float32) for count in pivots]
    scratch += [
        pltpu.VMEM((GROUPS, 2, width, max(pivots)), jnp.float32),
        pltpu.VMEM((GROUPS, 2, 2, width, max(pivots)), jnp.float32),
    ]
    lane_blocks = [count // 2 for count in blocks]
    landing = []
    for height, count in enumerate(lane_blocks):
        kept = kept_blocks(front_bits, height, count)
        landing.append(count - kept + 2 * swap_steps(height) * kept)
    for count in lane_blocks + landing + lane_blocks[1:]:
        scratch += stripe_buffers(count)
    scratch += [pltpu.SemaphoreType.DMA((2,)) for _ in range(3)]
    scratch += [pltpu.SemaphoreType.REGULAR]
    scratch += [pltpu.SemaphoreType.DMA((count,)) for count in (GROUPS, 2 * GROUPS)]
    scratch += [pltpu.SemaphoreType.DMA((count,)) for count in (len(stripe_rows), roles * len(stripe_rows))]
    scratch += [pltpu.SemaphoreType.DMA((1,)) for _ in range(4)]
    vmem = pl.BlockSpec(memory_space=pltpu.VMEM)
    smem = pl.BlockSpec(memory_space=pltpu.SMEM)
    out = pl.pallas_call(
        functools.partial(solve_kernel, leaf_bits, front_bits, stripe_rows, pivots, sizes, cap),
        out_shape=jax.ShapeDtypeStruct((rows // 8, 8, rhs_count), jnp.float32),
        in_specs=[vmem] + [smem] * 4 + [pl.BlockSpec(memory_space=pl.ANY)] * 7,
        out_specs=vmem,
        scratch_shapes=scratch,
        compiler_params=pltpu.CompilerParams(
            collective_id=0, has_side_effects=True, vmem_limit_bytes=66 * 1024 * 1000
        ),
    )(app_rhs.reshape(rows, 1, rhs_count), *tables, *weights)
    return out.reshape(rows, rhs_count)


def slots_of(owner, order, row_count, cap):
    block = owner // row_count
    before = (block[:, None] == block[None, :]) & (order[None, :] < order[:, None])
    return block * cap + jnp.sum(before.astype(jnp.int32), axis=1)


def rows_of(slots, slot_count):
    rows = jnp.arange(slots.shape[0], dtype=jnp.int32)
    same = jnp.arange(slot_count, dtype=jnp.int32)[:, None] == slots[None, :]
    return jnp.sum(jnp.where(same, rows[None, :], 0), axis=1)


def per_device(app_rhs, pivot_source, row_owner, *matrices):
    row_count = app_rhs.shape[0]
    peer_count = lax.axis_size("leaf") * lax.axis_size("front")
    mean_rows = row_count // (peer_count // 2)
    cap = mean_rows + max(1, mean_rows // 4)
    send_slots = slots_of(row_owner, jnp.arange(row_count, dtype=jnp.int32), row_count, cap)
    recv_slots = slots_of(pivot_source, pivot_source, row_count, cap)
    tables = (
        rows_of(send_slots, peer_count * cap),
        recv_slots,
        rows_of(recv_slots, peer_count * cap),
        send_slots,
    )
    return solve(app_rhs, tables, [w[0, 0] for w in matrices], cap)


def solution(mesh):
    rows = P(("leaf", "front"), None)
    flat = P(("leaf", "front"))
    blocks = P("leaf", "front", None, None)
    return jax.shard_map(
        per_device, mesh=mesh, in_specs=(rows, flat, flat) + (blocks,) * 7, out_specs=rows, check_vma=False
    )
```

```python
import functools

import jax
import jax.numpy as jnp
from jax import lax
from jax.experimental import pallas as pl
from jax.experimental.pallas import tpu as pltpu
from jax.sharding import PartitionSpec as P

BLK = 128
HEIGHTS = 4
CLASSES = 3
MESH = pl.DeviceIdType.MESH
CORE = ("front", 0)
GROUPS = 2
STRIPE_UNITS = (1,) * 8


def bit_of(value, place):
    return lax.rem(lax.div(value, jnp.int32(2**place)), jnp.int32(2))


def flipped(value, mask, bits):
    out = jnp.int32(0)
    for place in range(bits):
        out = out + lax.rem(bit_of(value, place) + bit_of(mask, place), jnp.int32(2)) * 2**place
    return out


def group_dims(front_bits, height):
    return [("front", place) for place in range(1, front_bits)] + [("leaf", place) for place in range(height)]


def group_orders(front_bits, height):
    dims = group_dims(front_bits, height)
    turns = min(CLASSES, len(dims))
    head, rest = dims[:turns], dims[turns:]
    return [head[turn:] + head[:turn] + rest for turn in range(turns)]


def swap_steps(height):
    return (0, 2, 2, 1)[height]


def kept_blocks(front_bits, height, half):
    return half >> (len(group_dims(front_bits, height)) - swap_steps(height))


def place_slot(place, height, order):
    slot = 0
    for axis, at in order:
        slot = slot * 2 + (place >> (at + height if axis == "front" else at) & 1)
    return slot


def place_lane(place):
    return bin(place).count("1") % 2


def split(value):
    high = value.astype(jnp.bfloat16)
    return high, (value - high.astype(jnp.float32)).astype(jnp.bfloat16)


def dot(left, right, right_axis):
    dims = (((1,), (right_axis,)), ((), ()))
    return lax.dot_general(left, right, dimension_numbers=dims, preferred_element_type=jnp.float32)


def solve_kernel(leaf_bits, front_bits, stripe_rows, pivots, sizes, cap, *refs):
    app_ref, pack_idx, order_idx, back_pack_idx, back_idx = refs[:5]
    weights_hbm = refs[5:12]
    out_ref = refs[12]
    packed, arrived, returned, ordered, sol, right_ref, done_ref = refs[13:20]
    near, far = refs[20:22]
    stacked = refs[22:29]
    left_ref = refs[29]
    solved = refs[30:34]
    pair_out, pair_in = refs[34:36]
    buffers = refs[36:-12]
    near_sems, far_send, far_recv, free_sem, pair_send, pair_recv = refs[-12:-6]
    send_sems, recv_sems, go_send, go_recv, back_send, back_recv = refs[-6:]
    stripes = len(stripe_rows)
    per_group = stripes // GROUPS
    width = sum(stripe_rows[:per_group])
    lows = [sum(stripe_rows[:s]) % width for s in range(stripes)]
    pos = 0

    def take(count):
        nonlocal pos
        pos += count
        return buffers[pos - count : pos]

    partial = [take(stripes) for _ in range(HEIGHTS)]
    recv = [take(stripes) for _ in range(HEIGHTS)]
    whole_vec = [partial[0]] + [take(stripes) for _ in range(HEIGHTS - 1)]

    leaf = lax.axis_index("leaf")
    front = lax.axis_index("front")
    fronts = 2**front_bits
    peers = 2 ** (front_bits + leaf_bits)
    here = {"leaf": leaf, "front": front}
    me = leaf * fronts + front

    def mine(dim):
        return bit_of(here[dim[0]], dim[1])

    core_flip = front + (1 - 2 * mine(CORE))

    def partner(dim):
        axis, place = dim
        if dim == CORE:
            return (leaf, core_flip)
        move = (1 - 2 * mine(dim)) * 2**place
        return (leaf + move, core_flip) if axis == "leaf" else (leaf, core_flip + move)

    def peer(step):
        turn = jnp.int32(peers - 1) - step
        return (
            flipped(leaf, lax.div(turn, jnp.int32(fronts)), leaf_bits),
            flipped(front, lax.rem(turn, jnp.int32(fronts)), front_bits),
        )

    piece_of = [pivots[h] // BLK for h in range(HEIGHTS)]
    halves = [size // BLK // 2 for size in sizes]
    orders = [group_orders(front_bits, h) for h in range(HEIGHTS)]
    lanes = []
    for height in range(HEIGHTS):
        total = jnp.int32(0)
        for place in range(front_bits):
            total = total + bit_of(front, place)
        for place in range(height):
            total = total + bit_of(leaf, place)
        lanes.append(lax.rem(total, jnp.int32(2)))

    def kind(height, stripe):
        return stripe % per_group % len(orders[height])

    places = []
    for height in range(HEIGHTS):
        table = {}
        for place in range(2 ** (front_bits + height)):
            if not place >> height & 1:
                table[place_slot(place, height, orders[height][0])] = place
        places.append(table)

    perms = []
    for height in range(HEIGHTS):
        table = [[0] * halves[height] for _ in orders[height]]
        for place in range(2 ** (front_bits + height)):
            canon = place_slot(place, height, orders[height][0])
            for k, order in enumerate(orders[height]):
                for part in range(piece_of[height]):
                    table[k][canon * piece_of[height] + part] = (
                        place_slot(place, height, order) * piece_of[height] + part
                    )
        perms.append(table)

    weight_heights = (0, 1, 1, 2, 2, 3, 3)
    pieces = []
    for index in range(7):
        for part in range(weights_hbm[index].shape[0] // BLK):
            pieces.append((index, part))

    def column(height, at, lane):
        piece = piece_of[height]
        place, rest = places[height][at // piece], at % piece
        core = lax.rem(lane + place_lane(place), jnp.int32(2))
        return pl.multiple_of((place * piece + rest) * BLK + core * (2**height * piece * BLK), BLK)

    def block_copies(number, lane):
        index, part = pieces[number]
        height = weight_heights[index]
        for at in range(halves[height]):
            yield at, weights_hbm[index].at[pl.ds(part * BLK, BLK), pl.ds(column(height, at, lane), BLK)]

    def start_near(number):
        for at, source in block_copies(number, lanes[weight_heights[pieces[number][0]]]):
            pltpu.make_async_copy(source, near.at[number % 2, at], near_sems.at[number % 2]).start()

    def far_copy(number, at, source):
        return pltpu.make_async_remote_copy(
            src_ref=source,
            dst_ref=at,
            send_sem=far_send.at[number % 2],
            recv_sem=far_recv.at[number % 2],
            device_id=(leaf, core_flip),
            device_id_type=MESH,
        )

    def start_far(number):
        for at, source in block_copies(number, 1 - lanes[weight_heights[pieces[number][0]]]):
            far_copy(number, far.at[number % 2, at], source).start()

    start_near(0)
    start_near(1)

    barrier = pltpu.get_barrier_semaphore()

    def greet(step):
        pl.semaphore_signal(barrier, inc=1, device_id=peer(step), device_id_type=MESH)


    def pack_rows(index, source, target, base, where):
        for row in range(cap):
            target[base + row] = source(index[where + row])

    def send_to(step, source, target, sends, recvs):
        to_leaf, to_front = peer(step)
        there = to_leaf * fronts + to_front
        return pltpu.make_async_remote_copy(
            src_ref=source.at[pl.ds(there * cap, cap)],
            dst_ref=target.at[pl.ds(me * cap, cap)],
            send_sem=sends.at[0],
            recv_sem=recvs.at[0],
            device_id=(to_leaf, to_front),
            device_id_type=MESH,
        )

    def exchange_rows(index, source, target, sends, recvs, ready):
        def pack(step):
            to_leaf, to_front = peer(step)
            base = (to_leaf * fronts + to_front) * cap
            pack_rows(index, source, packed, base, base)

        if ready is not None:

            def meet(step, carry):
                greet(step)
                pack(step)
                return carry

            lax.fori_loop(0, peers - 1, meet, 0)
            pack_rows(index, source, target, me * cap, me * cap)
            ready()

            def launch(step, carry):
                send_to(step, packed, target, sends, recvs).start()
                return carry

            lax.fori_loop(0, peers - 1, launch, 0)
            return

        pack(jnp.int32(0))

        def body(step, carry):
            pack(step)
            send_to(step - 1, packed, target, sends, recvs).start()
            return carry

        lax.fori_loop(1, peers - 1, body, 0)
        pack_rows(index, source, target, me * cap, me * cap)
        send_to(jnp.int32(peers - 2), packed, target, sends, recvs).start()

    def finish_rows(target, sends, recvs):
        for ref, sem in ((packed, sends), (target, recvs)):
            span = ref.at[pl.ds(0, (peers - 1) * cap)]
            pltpu.make_async_copy(span, span, sem.at[0]).wait()

    def unpack_rows(index, source, target):
        def body(group, carry):
            for row in range(8):
                target[group, pl.ds(row, 1), :] = source[index[group * 8 + row]]
            return carry

        lax.fori_loop(0, target.shape[0], body, 0, unroll=2)

    exchange_rows(
        pack_idx,
        lambda i: app_ref[i],
        arrived,
        go_send,
        go_recv,
        lambda: pl.semaphore_wait(barrier, peers - 1),
    )
    start_far(0)
    start_far(1)

    for number, (index, part) in enumerate(pieces):
        rows = weights_hbm[index].shape[0]
        half = halves[weight_heights[index]]
        slot = number % 2
        here_all, there_all = near.at[slot, pl.ds(0, half)], far.at[slot, pl.ds(0, half)]
        pltpu.make_async_copy(here_all, here_all, near_sems.at[slot]).wait()
        far_copy(number, there_all, there_all).wait()

        def convert(group, carry, index=index, part=part, rows=rows, half=half, slot=slot):
            span = pl.ds(pl.multiple_of(group * 16, 16), 16)
            for side, source in enumerate((near, far)):
                for at in range(half):
                    for level, value in enumerate(split(source[slot, at, span, :])):
                        start = (2 * side + level) * rows + part * BLK + group * 16
                        stacked[index][pl.ds(pl.multiple_of(start, 16), 16), pl.ds(at * BLK, BLK)] = value
            return carry

        lax.fori_loop(0, BLK // 16, convert, 0)
        if number + 2 < len(pieces):
            pl.semaphore_signal(free_sem, inc=1, device_id=(leaf, core_flip), device_id_type=MESH)
            start_near(number + 2)
            pl.semaphore_wait(free_sem, 1)
            start_far(number + 2)

    finish_rows(arrived, go_send, go_recv)
    unpack_rows(order_idx, arrived, ordered)

    all_dims = group_dims(front_bits, leaf_bits)

    def remote(source, target, dim, stripe, role):
        if role < 2:
            role = role * len(all_dims) + all_dims.index(dim)
        else:
            role = role - 2 + 2 * len(all_dims)
        index = role * stripes + stripe
        copy = pltpu.make_async_remote_copy(
            src_ref=source,
            dst_ref=target,
            send_sem=send_sems.at[stripe],
            recv_sem=recv_sems.at[index],
            device_id=partner(dim),
            device_id_type=MESH,
        )
        copy.start()
        return copy

    def members(group):
        return range(group * per_group, (group + 1) * per_group)

    def own_slot(height, stripe):
        slot = jnp.int32(0)
        for dim in orders[height][kind(height, stripe)]:
            slot = slot * 2 + mine(dim)
        return slot * piece_of[height]

    def reduce_steps(group, height, way, bases):
        bufs, recvs, result = partial[height], recv[height], whole_vec[height]
        depth = len(orders[height][0])
        whole, prior, offset = halves[height], 0, 0
        swaps = swap_steps(height)
        kept = kept_blocks(front_bits, height, whole)
        pending = {}
        for step in range(depth + 1):
            full = depth - swaps <= step
            size = whole if full else whole // 2
            number = way * swaps + step - depth + swaps
            if full:
                offset = halves[height] - kept + number * kept
            if step > 0:
                yield
            for s in members(group):
                if step > 0:
                    pending[s].wait()
                    keep = pl.ds(bases[s], whole)
                    (result if step == depth else bufs)[s][keep] = bufs[s][keep] + recvs[s][pl.ds(prior, whole)]
                if step < depth:
                    dim = orders[height][kind(height, s)][step]
                    away, role = bases[s], 0
                    if full:
                        role = 2 * height + (way if height == HEIGHTS - 1 else number % swaps)
                    else:
                        away = bases[s] + (1 - mine(dim)) * size
                        bases[s] = bases[s] + mine(dim) * size
                    pending[s] = remote(
                        bufs[s].at[pl.ds(away, size)], recvs[s].at[pl.ds(offset, size)], dim, s, role
                    )
            prior, whole = offset, size
            offset += size

    def gather_steps(group, height, bases, size, depth):
        bufs = whole_vec[height]
        pending = {}
        for step in range(depth - 1, -1, -1):
            for s in members(group):
                if pending.get(s) is not None:
                    pending[s].wait()
                dim = orders[height][kind(height, s)][step]
                span = pl.ds(bases[s], size)
                pending[s] = remote(bufs[s].at[span], bufs[s].at[span], dim, s, 1)
                bases[s] = bases[s] - mine(dim) * size
            size *= 2
            yield
        for copy in pending.values():
            copy.wait()

    def spread_steps(group, height, bases):
        kept = kept_blocks(front_bits, height, halves[height])
        return gather_steps(group, height, bases, kept, len(orders[height][0]) - swap_steps(height))

    turns = [0] * GROUPS

    def apply_rows(group, index, height, finish):
        bufs, half = whole_vec[height], halves[height]
        for at in range(half):
            block = jnp.concatenate(
                [bufs[s][perms[height][kind(height, s)][at]] for s in members(group)], axis=0
            )
            high, low = split(block)
            left_ref[0:width, at * BLK : (at + 1) * BLK] = high
            left_ref[width : 2 * width, at * BLK : (at + 1) * BLK] = low
        full = dot(left_ref[:, 0 : half * BLK], stacked[index][...], 1)
        both = full[:width] + full[width:]
        rows = both.shape[1] // 4
        turn = turns[group] % 2
        turns[group] += 1
        for side in range(2):
            low = 2 * side * rows
            pair_out[group, side, :, 0:rows] = both[:, low : low + rows] + both[:, low + rows : low + 2 * rows]
        copy = pltpu.make_async_remote_copy(
            src_ref=pair_out.at[group, :, :, pl.ds(0, rows)],
            dst_ref=pair_in.at[group, turn, :, :, pl.ds(0, rows)],
            send_sem=pair_send.at[group],
            recv_sem=pair_recv.at[2 * group + turn],
            device_id=(leaf, core_flip),
            device_id_type=MESH,
        )
        copy.start()
        yield
        copy.wait()
        finish(
            jnp.concatenate(
                [pair_out[group, side, :, 0:rows] + pair_in[group, turn, 1 - side, :, 0:rows] for side in range(2)],
                axis=1,
            )
        )

    def apply_cols(group, index, height, vector):
        bufs, half = partial[height], halves[height]
        rows = vector.shape[1] // 2
        sides = []
        for part in split(vector):
            near_part, far_part = part[:, :rows], part[:, rows:]
            sides.append(jnp.concatenate([near_part, near_part, far_part, far_part], axis=1))
        left = jnp.concatenate(sides, axis=0)
        for at in range(0, half, 2):
            full = dot(left, stacked[index][:, at * BLK : (at + 2) * BLK], 0)
            both = full[:width] + full[width:]
            for step in range(2):
                for s in members(group):
                    bufs[s][perms[height][kind(height, s)][at + step]] = both[
                        lows[s] : lows[s] + stripe_rows[s], step * BLK : (step + 1) * BLK
                    ]

    inverses = (0, 2, 4, 6)
    couplings = (1, 3, 5)
    starts = [sum(pivots[:h]) // BLK for h in range(HEIGHTS)]
    for part in range(right_ref.shape[0]):
        low = part * BLK // 8
        right_ref[part] = ordered[low : low + BLK // 8].reshape(BLK, -1).T

    def chain(group):
        def keep_value(height):
            def keep(value):
                solved[height][group] = value

            return keep

        def own_right(height, part, s):
            low = group * width + lows[s]
            return right_ref[starts[height] + part, low : low + stripe_rows[s]]

        bases = {s: own_slot(0, s) for s in members(group)}
        for part in range(piece_of[0]):
            for s in members(group):
                partial[0][s][bases[s] + part] = own_right(0, part, s)
        yield from gather_steps(group, 0, bases, piece_of[0], len(orders[0][0]))
        yield from apply_rows(group, inverses[0], 0, keep_value(0))
        for height in range(1, HEIGHTS):
            apply_cols(group, couplings[height - 1], height, -solved[height - 1][group])
            for s in members(group):
                spot, slot = partial[height][s], own_slot(height, s)
                spot[slot] = spot[slot] + own_right(height, 0, s)
            bases = dict.fromkeys(members(group), 0)
            yield from reduce_steps(group, height, 0, bases)
            yield from spread_steps(group, height, bases)
            yield from apply_rows(group, inverses[height], height, keep_value(height))
        target = [solved[HEIGHTS - 1][group]]
        for height in range(HEIGHTS - 1, -1, -1):
            apply_cols(group, inverses[height], height, target.pop())
            bases = dict.fromkeys(members(group), 0)
            yield from reduce_steps(group, height, 1, bases)
            for part in range(piece_of[height]):
                for s in members(group):
                    low = group * width + lows[s]
                    done_ref[starts[height] + part, low : low + stripe_rows[s]] = whole_vec[height][s][
                        own_slot(height, s) + part
                    ]
            if height > 0:
                yield from spread_steps(group, height, bases)
                yield from apply_rows(
                    group,
                    couplings[height - 1],
                    height,
                    lambda value: target.append(solved[height - 1][group] - value),
                )

    chains = [chain(group) for group in range(GROUPS)]
    while chains:
        for running in list(chains):
            if next(running, chains) is chains:
                chains.remove(running)
    for part in range(done_ref.shape[0]):
        sol[part * BLK : (part + 1) * BLK, :] = done_ref[part].T

    exchange_rows(
        back_pack_idx, lambda i: sol[pl.ds(i, 1), :], returned, back_send, back_recv, None
    )
    finish_rows(returned, back_send, back_recv)
    unpack_rows(back_idx, returned, out_ref)


def solve(app_rhs, tables, weights, cap):
    leaves = lax.axis_size("leaf")
    fronts = lax.axis_size("front")
    peers = leaves * fronts
    front_bits = fronts.bit_length() - 1
    leaf_bits = leaves.bit_length() - 1
    rows, rhs_count = app_rhs.shape
    units = [unit * rhs_count // BLK for unit in STRIPE_UNITS * GROUPS]
    width = rhs_count // GROUPS
    stripe_rows = tuple(8 * unit for unit in units)
    inverses = (weights[0], weights[2], weights[4], weights[6])
    sizes = tuple(w.shape[1] for w in inverses)
    pivots = tuple(w.shape[0] for w in inverses)
    blocks = [size // BLK for size in sizes]

    def stripe_buffers(count):
        return [pltpu.VMEM((count, height, BLK), jnp.float32) for height in stripe_rows]

    roles = 2 * len(group_dims(front_bits, leaf_bits)) + 2 * (HEIGHTS - 1)
    scratch = [
        pltpu.VMEM((peers * cap, 1, rhs_count), jnp.float32),
        pltpu.VMEM((peers * cap, 1, rhs_count), jnp.float32),
        pltpu.VMEM((peers * cap, 1, rhs_count), jnp.float32),
        pltpu.VMEM((rows // 8, 8, rhs_count), jnp.float32),
        pltpu.VMEM((rows, rhs_count), jnp.float32),
        pltpu.VMEM((rows // BLK, rhs_count, BLK), jnp.float32),
        pltpu.VMEM((rows // BLK, rhs_count, BLK), jnp.float32),
        pltpu.VMEM((2, max(blocks) // 2, BLK, BLK), jnp.float32),
        pltpu.VMEM((2, max(blocks) // 2, BLK, BLK), jnp.float32),
    ]
    scratch += [pltpu.VMEM((4 * w.shape[0], w.shape[1] // 2), jnp.bfloat16) for w in weights]
    scratch += [pltpu.VMEM((2 * width, max(sizes) // 2), jnp.bfloat16)]
    scratch += [pltpu.VMEM((GROUPS, width, 2 * count), jnp.float32) for count in pivots]
    scratch += [
        pltpu.VMEM((GROUPS, 2, width, max(pivots)), jnp.float32),
        pltpu.VMEM((GROUPS, 2, 2, width, max(pivots)), jnp.float32),
    ]
    lane_blocks = [count // 2 for count in blocks]
    landing = []
    for height, count in enumerate(lane_blocks):
        kept = kept_blocks(front_bits, height, count)
        landing.append(count - kept + 2 * swap_steps(height) * kept)
    for count in lane_blocks + landing + lane_blocks[1:]:
        scratch += stripe_buffers(count)
    scratch += [pltpu.SemaphoreType.DMA((2,)) for _ in range(3)]
    scratch += [pltpu.SemaphoreType.REGULAR]
    scratch += [pltpu.SemaphoreType.DMA((count,)) for count in (GROUPS, 2 * GROUPS)]
    scratch += [pltpu.SemaphoreType.DMA((count,)) for count in (len(stripe_rows), roles * len(stripe_rows))]
    scratch += [pltpu.SemaphoreType.DMA((1,)) for _ in range(4)]
    vmem = pl.BlockSpec(memory_space=pltpu.VMEM)
    smem = pl.BlockSpec(memory_space=pltpu.SMEM)
    out = pl.pallas_call(
        functools.partial(solve_kernel, leaf_bits, front_bits, stripe_rows, pivots, sizes, cap),
        out_shape=jax.ShapeDtypeStruct((rows // 8, 8, rhs_count), jnp.float32),
        in_specs=[vmem] + [smem] * 4 + [pl.BlockSpec(memory_space=pl.ANY)] * 7,
        out_specs=vmem,
        scratch_shapes=scratch,
        compiler_params=pltpu.CompilerParams(
            collective_id=0, has_side_effects=True, vmem_limit_bytes=66 * 1024 * 1000
        ),
    )(app_rhs.reshape(rows, 1, rhs_count), *tables, *weights)
    return out.reshape(rows, rhs_count)


def slots_of(owners, row_count, cap):
    owners = lax.optimization_barrier(owners)
    block = lax.optimization_barrier(owners // row_count)
    sent = lax.broadcasted_iota(jnp.int32, owners.shape, 0) == 0
    order = jnp.where(sent, lax.broadcasted_iota(jnp.int32, owners.shape, 1), owners)
    before = (block[:, :, None] == block[:, None, :]) & (order[:, None, :] < order[:, :, None])
    return lax.optimization_barrier(block * cap + jnp.sum(before.astype(jnp.int32), axis=2))


def rows_of(slots, slot_count):
    rows = jnp.arange(slots.shape[1], dtype=jnp.int32)
    same = jnp.arange(slot_count, dtype=jnp.int32)[None, :, None] == slots[:, None, :]
    return jnp.sum(jnp.where(same, rows[None, None, :], 0), axis=2)


def per_device(app_rhs, pivot_source, row_owner, *matrices):
    row_count = app_rhs.shape[0]
    peer_count = lax.axis_size("leaf") * lax.axis_size("front")
    mean_rows = row_count // (peer_count // 2)
    cap = mean_rows + max(1, mean_rows // 4)
    slots = slots_of(jnp.stack([row_owner, pivot_source]), row_count, cap)
    rows = rows_of(slots, peer_count * cap)
    tables = (rows[0], slots[1], rows[1], slots[0])
    return solve(app_rhs, tables, [w[0, 0] for w in matrices], cap)


def solution(mesh):
    rows = P(("leaf", "front"), None)
    flat = P(("leaf", "front"))
    blocks = P("leaf", "front", None, None)
    return jax.shard_map(
        per_device, mesh=mesh, in_specs=(rows, flat, flat) + (blocks,) * 7, out_specs=rows, check_vma=False
    )
```
